32 devices in a mesh: rep: 1, dp: 32 (over x, y, z, core).
Axes of the slice: x: 2, y: 2, z: 4, core: 2. Of those that a mesh axis runs over, the one named last changes fastest.
Arguments:
- x: bfloat16 [32, 2048, 1024], P(('rep', 'dp'))
- dy: bfloat16 [32, 2048, 1024], P(('rep', 'dp'))
- w_gate: bfloat16 [2, 1024, 5120], replicated
- w_up: bfloat16 [2, 1024, 5120], replicated
- w_down: bfloat16 [2, 5120, 1024], replicated
- m_w_gate: float32 [2, 1024, 5120], replicated
- m_w_up: float32 [2, 1024, 5120], replicated
- m_w_down: float32 [2, 5120, 1024], replicated
- v_w_gate: float32 [2, 1024, 5120], replicated
- v_w_up: float32 [2, 1024, 5120], replicated
- v_w_down: float32 [2, 5120, 1024], replicated
Outputs:
- output 1: bfloat16 [2, 1024, 5120], P('rep')
- output 2: bfloat16 [2, 1024, 5120], P('rep')
- output 3: bfloat16 [2, 5120, 1024], P('rep')
- output 4: float32 [2, 1024, 5120], P('rep')
- output 5: float32 [2, 1024, 5120], P('rep')
- output 6: float32 [2, 5120, 1024], P('rep')
- output 7: float32 [2, 1024, 5120], P('rep')
- output 8: float32 [2, 1024, 5120], P('rep')
- output 9: float32 [2, 5120, 1024], P('rep')
All inputs are finite; a program needn't handle non-finite values.
Results may differ from the reference program's by a relative error of at most 0.022.
Values are sent between devices in bfloat16 or wider.
A program may use at most 3 GiB of HBM per device.

```python
import jax
import jax.numpy as jnp
from jax import lax

SEQUENCES = 32
TOKENS = 2048
D = 1024
FF = 5120
LAYERS = 2
NAMES = ("w_gate", "w_up", "w_down")
SHAPES = {"w_gate": (LAYERS, D, FF), "w_up": (LAYERS, D, FF), "w_down": (LAYERS, FF, D)}


def bump(key, n, height):
    away = (jnp.arange(n, dtype=jnp.int32) - jax.random.randint(key, (), 0, n, jnp.int32)) % n
    return jnp.where(away < n // 8, height, 1.0)


def together(key, own, strength):
    shared = jax.random.normal(key, own.shape[1:], jnp.float32)
    return (own + strength * shared) * lax.rsqrt(1 + strength * strength)


def setup_inputs(seed: int = 0, part: int = 0) -> dict:
    kx, kdy, ka, kb, kz, kf, kh, kl, *keys = jax.random.split(jax.random.key(seed), 8 + 3 * len(NAMES))
    kx, kdy, ka, kb = (jax.random.fold_in(k, part) for k in (kx, kdy, ka, kb))
    kw, km, kv = (keys[i::3] for i in range(3))
    shape = (SEQUENCES, TOKENS, D)
    much_x, much_dy = jax.random.uniform(kz, (2,), jnp.float32, 0.0, 1.0)
    loud = 2.0 ** jax.random.uniform(jax.random.fold_in(kz, 1), (), jnp.float32, -1.0, 2.0)
    layers = 2.0 ** jax.random.uniform(kl, (LAYERS, 1, 1), jnp.float32, -1.0, 1.0)
    x = together(ka, jax.random.normal(kx, shape, jnp.float32), much_x) * bump(kf, D, 4.0)
    dy = together(kb, jax.random.normal(kdy, shape, jnp.float32), much_dy)
    drawn = {"x": x.astype(jnp.bfloat16), "dy": (loud * dy * (SEQUENCES * TOKENS) ** -0.5).astype(jnp.bfloat16)}
    for key, name in zip(kw, NAMES, strict=True):
        w = jax.random.normal(key, SHAPES[name], jnp.float32) * SHAPES[name][1] ** -0.5
        drawn[name] = (w * {"w_gate": 1.0, "w_up": bump(kh, FF, 4.0), "w_down": layers}[name]).astype(jnp.bfloat16)
    for key, name in zip(km, NAMES, strict=True):
        drawn[f"m_{name}"] = 0.1 * jax.random.normal(key, SHAPES[name], jnp.float32)
    for key, name in zip(kv, NAMES, strict=True):
        drawn[f"v_{name}"] = jax.random.uniform(key, SHAPES[name], jnp.float32, 0.005, 0.015)
    return drawn


def matmul(a, w):
    return jnp.dot(a, w, preferred_element_type=jnp.float32).astype(jnp.bfloat16)


def normed(h):
    wide = h.astype(jnp.float32)
    scale = lax.rsqrt(jnp.mean(wide**2, -1, keepdims=True) + 1e-6)
    return (wide * scale).astype(jnp.bfloat16)


def layer(h, w):
    a = normed(h)
    gate = jnp.dot(a, w["w_gate"], preferred_element_type=jnp.float32)
    up = jnp.dot(a, w["w_up"], preferred_element_type=jnp.float32)
    return h + matmul((jax.nn.silu(gate) * up).astype(jnp.bfloat16), w["w_down"])


def adamw(w, m, v, g):
    m = 0.9 * m + 0.1 * g
    v = 0.95 * v + 0.05 * g * g
    step = m * lax.rsqrt(v + 1e-8) + 0.1 * w
    return (w - 0.02 * step).astype(jnp.bfloat16), m, v


def stack(weights, h):
    return lax.scan(lambda h, w: (layer(h, w), None), h, weights)[0]


def reference(x, dy, w_gate, w_up, w_down, m_w_gate, m_w_up, m_w_down, v_w_gate, v_w_up, v_w_down):
    weights = dict(zip(NAMES, (w_gate, w_up, w_down), strict=True))

    def take(so_far, sequence):
        h, by_y = sequence
        _, back = jax.vjp(lambda w: stack(w, h), weights)
        return jax.tree.map(lambda total, term: total + term.astype(jnp.float32), so_far, back(by_y)[0]), None

    none_yet = {name: jnp.zeros(w.shape, jnp.float32) for name, w in weights.items()}
    by_weights, _ = lax.scan(take, none_yet, (x, dy))
    gradients = [by_weights[name].astype(jnp.bfloat16).astype(jnp.float32) for name in NAMES]
    new = [
        adamw(w.astype(jnp.float32), m, v, g)
        for w, m, v, g in zip((w_gate, w_up, w_down), (m_w_gate, m_w_up, m_w_down), (v_w_gate, v_w_up, v_w_down), gradients, strict=True)
    ]
    return tuple(one[which] for which in range(3) for one in new)
```

```python
import functools

import jax
import jax.numpy as jnp
from jax import lax
from jax.experimental import pallas as pl
from jax.experimental.pallas import tpu as pltpu
from jax.sharding import PartitionSpec as P

MESH = pl.DeviceIdType.MESH
F32, BF16 = jnp.float32, jnp.bfloat16
MIB = 1024 * 1024

CORE, Z0, Z1, Y, X = 1, 2, 4, 8, 16
BITS = (CORE, Z0, Z1, Y, X)
ORDERS = ((CORE, X, Y, Z0, Z1), (CORE, Y, X, Z0, Z1), (CORE, Z0, X, Y, Z1))
STAGES = 5
GROUP = 1 << STAGES
CHUNK = 512
LAG = 2
SLOTS = 2 * LAG
R_SLOTS = 16


def pick(color, values):
    out = values[-1]
    for k in range(len(values) - 2, -1, -1):
        out = jnp.where(color == k, values[k], out)
    return out


def position(order, device):
    return sum(((device // m) % 2) << (STAGES - 1 - i) for i, m in enumerate(order))


def owners(order):
    found = [0] * GROUP
    for device in range(GROUP):
        found[position(order, device)] = device
    return found


def params(limit=60, **more):
    return pltpu.CompilerParams(dimension_semantics=("arbitrary",), vmem_limit_bytes=limit * MIB, **more)


def dot(a, b):
    return jnp.dot(a, b, preferred_element_type=F32)


def dot_nt(a, b):
    return lax.dot_general(a, b, (((1,), (1,)), ((), ())), preferred_element_type=F32)


def once(shape, index):
    return pl.BlockSpec(shape, index, pipeline_mode=pl.Buffered(1))


def norm_in(h):
    wide = h.astype(F32)
    return (wide * lax.rsqrt(jnp.mean(wide**2, -1, keepdims=True) + 1e-6)).astype(BF16)


def normed(h):
    wide = h.astype(F32)
    scale = lax.rsqrt(jnp.mean(wide**2, -1, keepdims=True) + 1e-6)
    return (wide * scale).astype(BF16)


def forward_kernel(parts, h_ref, wg_ref, wu_ref, gate_ref, up_ref, mid_ref, a_ref):
    t = h_ref.shape[0] // parts

    @pl.when(pl.program_id(0) == 0)
    def _():
        for i in range(parts):
            a_ref[i * t : (i + 1) * t] = norm_in(h_ref[i * t : (i + 1) * t])

    for i in range(parts):
        rows = slice(i * t, (i + 1) * t)
        gate = dot(a_ref[rows], wg_ref[0])
        up = dot(a_ref[rows], wu_ref[0])
        gate_ref[rows] = gate
        up_ref[rows] = up
        mid_ref[rows] = (jax.nn.silu(gate) * up).astype(BF16)


def forward(h, w_gate, w_up, layer):
    tokens, d = h.shape
    ff = w_gate.shape[2]
    weight = pl.BlockSpec((1, d, CHUNK), lambda j: (layer, 0, j))
    tile = pl.BlockSpec((tokens, CHUNK), lambda j: (0, j))
    return pl.pallas_call(
        functools.partial(forward_kernel, 4),
        grid=(ff // CHUNK,),
        in_specs=[once((tokens, d), lambda j: (0, 0)), weight, weight],
        out_specs=[tile, tile, tile],
        out_shape=[jax.ShapeDtypeStruct((tokens, ff), t) for t in (F32, F32, BF16)],
        scratch_shapes=[pltpu.VMEM((tokens, d), BF16)],
        compiler_params=params(),
        cost_estimate=pl.CostEstimate(flops=4 * tokens * d * ff, bytes_accessed=10 * tokens * ff, transcendentals=tokens * ff),
        name="forward",
    )(h, w_gate, w_up)


def down_kernel(mid_ref, w_ref, h_ref, out_ref):
    out_ref[...] = h_ref[...] + dot(mid_ref[...], w_ref[0]).astype(BF16)


def down(mid, w_down, h, layer):
    tokens, ff = mid.shape
    d = h.shape[1]
    rows = 256
    return pl.pallas_call(
        down_kernel,
        grid=(tokens // rows,),
        in_specs=[
            pl.BlockSpec((rows, ff), lambda i: (i, 0)),
            once((1, ff, d), lambda i: (layer, 0, 0)),
            pl.BlockSpec((rows, d), lambda i: (i, 0)),
        ],
        out_specs=pl.BlockSpec((rows, d), lambda i: (i, 0)),
        out_shape=jax.ShapeDtypeStruct((tokens, d), BF16),
        compiler_params=params(),
        cost_estimate=pl.CostEstimate(flops=2 * tokens * d * ff, bytes_accessed=2 * (tokens + d) * ff, transcendentals=0),
        name="down",
    )(mid, w_down, h)


def through(gate, up, by_mid):
    by_mid = by_mid.astype(BF16).astype(F32)
    s = jax.nn.sigmoid(gate)
    silu = gate * s
    return (silu * up).astype(BF16), (by_mid * up * (s * (1 + gate * (1 - s)))).astype(BF16), (by_mid * silu).astype(BF16)


def turned(j, out_ref, first_ref, second_ref):
    width = out_ref.shape[1]
    at = lax.rem(j, 4) * width

    @pl.when(j < 4)
    def _():
        out_ref[0] = first_ref[:, pl.ds(pl.multiple_of(at, width), width)].T

    @pl.when((j >= 4) & (j < 8))
    def _():
        out_ref[0] = second_ref[:, pl.ds(pl.multiple_of(at, width), width)].T


def last_kernel(parts, h_ref, dy_ref, wg_ref, wu_ref, wd_ref, b_ref, at_ref, a_ref):
    t = h_ref.shape[0] // parts
    j = pl.program_id(0)

    @pl.when(j == 0)
    def _():
        for i in range(parts):
            a_ref[i * t : (i + 1) * t] = norm_in(h_ref[i * t : (i + 1) * t])

    turned(j, at_ref, dy_ref, a_ref)
    for i in range(parts):
        rows = slice(i * t, (i + 1) * t)
        gate = dot(a_ref[rows], wg_ref[0])
        up = dot(a_ref[rows], wu_ref[0])
        by_mid = dot_nt(dy_ref[rows], wd_ref[0])
        b_ref[0, rows], b_ref[1, rows], b_ref[2, rows] = through(gate, up, by_mid)


def middle_kernel(parts, h_ref, dy_ref, gate_ref, up_ref, wd_ref, b_ref, at_ref, a_ref):
    t = h_ref.shape[0] // parts
    j = pl.program_id(0)

    @pl.when(j == 0)
    def _():
        for i in range(parts):
            a_ref[i * t : (i + 1) * t] = norm_in(h_ref[i * t : (i + 1) * t])

    turned(j, at_ref, dy_ref, a_ref)
    for i in range(parts):
        rows = slice(i * t, (i + 1) * t)
        by_mid = dot_nt(dy_ref[rows], wd_ref[0])
        b_ref[0, rows], b_ref[1, rows], b_ref[2, rows] = through(gate_ref[rows], up_ref[rows], by_mid)


def backward_mid(h, dy, layer, w_down, kept=None, weights=None):
    tokens, d = h.shape
    ff = w_down.shape[1]
    whole = once((tokens, d), lambda j: (0, 0))
    tile = pl.BlockSpec((tokens, CHUNK), lambda j: (0, j))
    weight = pl.BlockSpec((1, d, CHUNK), lambda j: (layer, 0, j))
    turn = lambda j: (jnp.minimum(j // 4, 1), jnp.where(j < 8, lax.rem(j, 4), 3), 0)
    return pl.pallas_call(
        functools.partial(last_kernel if kept is None else middle_kernel, 4),
        grid=(ff // CHUNK,),
        in_specs=[whole, whole]
        + ([weight, weight] if kept is None else [tile, tile])
        + [pl.BlockSpec((1, CHUNK, d), lambda j: (layer, j, 0))],
        out_specs=[pl.BlockSpec((3, tokens, CHUNK), lambda j: (0, 0, j)), pl.BlockSpec((1, d // 4, tokens), turn)],
        out_shape=[jax.ShapeDtypeStruct((3, tokens, ff), BF16), jax.ShapeDtypeStruct((2, d, tokens), BF16)],
        scratch_shapes=[pltpu.VMEM((tokens, d), BF16)],
        compiler_params=params(),
        cost_estimate=pl.CostEstimate(
            flops=(6 if kept is None else 2) * tokens * d * ff, bytes_accessed=14 * tokens * ff, transcendentals=tokens * ff
        ),
        name="last" if kept is None else "middle",
    )(h, dy, *(weights if kept is None else kept), w_down)


def gradient_kernel(n_c, per, with_da, *refs):
    at_ref, b_ref = refs[:2]
    refs = refs[2:]
    if with_da:
        wg_ref, wu_ref, out_ref, da_ref = refs[:4]
        refs = refs[4:]
    else:
        out_ref = refs[0]
        refs = refs[1:]
    s_refs, k_refs, r_refs = refs[:STAGES], refs[STAGES : 2 * STAGES], refs[2 * STAGES : 3 * STAGES]
    send_sem, recv_sem = refs[3 * STAGES : 3 * STAGES + 2]
    rows = out_ref.shape[1]
    j = pl.program_id(0)
    me = lax.axis_index("dp")
    bits = {m: lax.rem(lax.div(me, m), 2) for m in BITS}
    peers = {m: me + m * (1 - 2 * bits[m]) for m in BITS}

    @pl.when(j == 0)
    def _():
        barrier = pltpu.get_barrier_semaphore()
        for m in BITS:
            pl.semaphore_signal(barrier, inc=1, device_id={"dp": peers[m]}, device_id_type=MESH)
        pl.semaphore_wait(barrier, len(BITS))

    def copy(stage, c):
        slot = lax.rem(c, SLOTS)
        r_slot = lax.rem(c, R_SLOTS)
        return pltpu.make_async_remote_copy(
            src_ref=s_refs[stage].at[slot],
            dst_ref=r_refs[stage].at[r_slot],
            send_sem=send_sem.at[stage, slot],
            recv_sem=recv_sem.at[stage, r_slot],
            device_id={"dp": pick(lax.rem(c, len(ORDERS)), [peers[o[stage]] for o in ORDERS])},
            device_id_type=MESH,
        )

    for s in reversed(range(STAGES)):
        c = j - (s + 1) * LAG

        @pl.when((c >= 0) & (c < n_c))
        def _(s=s, c=c):
            k_slot = lax.rem(c, LAG + 1)
            r_slot = lax.rem(c, R_SLOTS)
            came = copy(s, c)
            came.wait_send()
            came.wait_recv()
            if s == STAGES - 1:
                out_ref[0] = (k_refs[s][k_slot] + r_refs[s][r_slot].astype(F32)).astype(BF16)
            else:
                half = 2 ** (STAGES - 2 - s) * rows
                bit = pick(lax.rem(c, len(ORDERS)), [bits[o[s + 1]] for o in ORDERS])
                give = pl.ds(pl.multiple_of((1 - bit) * half, half), half)
                keep = pl.ds(pl.multiple_of(bit * half, half), half)
                s_refs[s + 1][lax.rem(c, SLOTS)] = (k_refs[s][k_slot, give] + r_refs[s][r_slot, give].astype(F32)).astype(BF16)
                k_refs[s + 1][k_slot] = k_refs[s][k_slot, keep] + r_refs[s][r_slot, keep].astype(F32)
                copy(s + 1, c).start()

    @pl.when(j < n_c)
    def _():
        core = bits[CORE]
        s_refs[0][lax.rem(j, SLOTS)] = dot(at_ref[0, 1 - core], b_ref[0]).astype(BF16)
        copy(0, j).start()
        k_refs[0][lax.rem(j, LAG + 1)] = dot(at_ref[0, core], b_ref[0])

    if with_da:
        acc_ref, da_sem = refs[3 * STAGES + 2 :]
        parts = 4
        t = acc_ref.shape[0] // parts
        for first, w_ref, begin in ((True, wg_ref, per), (False, wu_ref, 2 * per)):

            @pl.when((j >= begin) & (j < begin + per))
            def _(first=first, w_ref=w_ref, begin=begin):
                for i in range(parts):
                    piece = slice(i * t, (i + 1) * t)
                    term = dot_nt(b_ref[0, piece], w_ref[0])
                    if first:

                        @pl.when(j == begin)
                        def _():
                            acc_ref[piece] = term

                        @pl.when(j > begin)
                        def _():
                            acc_ref[piece] += term

                    else:
                        acc_ref[piece] += term

        @pl.when(j == n_c)
        def _():
            pltpu.make_async_copy(acc_ref, da_ref, da_sem).start()

        @pl.when(j == n_c + STAGES * LAG - 1)
        def _():
            pltpu.make_async_copy(acc_ref, da_ref, da_sem).wait()


def gradients(at, b, collective_id, layer, weights=None):
    _, d, tokens = at.shape
    w, _, ff = b.shape
    per = ff // CHUNK
    n_c = w * per
    rows = d // GROUP
    sizes = [2 ** (STAGES - 1 - s) * rows for s in range(STAGES)]
    clip = lambda j: jnp.minimum(j, n_c - 1)
    done = lambda j: jnp.clip(j - STAGES * LAG, 0, n_c - 1)
    with_da = weights is not None
    in_specs = [
        pl.BlockSpec((1, 2, d // 2, tokens), lambda j: (jnp.where(j < per, 0, 1), 0, 0, 0)),
        pl.BlockSpec((1, tokens, CHUNK), lambda j: (clip(j) // per, 0, lax.rem(clip(j), per))),
    ]
    out_specs = [pl.BlockSpec((1, rows, CHUNK), lambda j: (done(j) // per, 0, lax.rem(done(j), per)))]
    out_shape = [jax.ShapeDtypeStruct((w, rows, ff), BF16)]
    scratch = (
        [pltpu.VMEM((SLOTS, n, CHUNK), BF16) for n in sizes]
        + [pltpu.VMEM((LAG + 1, n, CHUNK), F32) for n in sizes]
        + [pltpu.VMEM((R_SLOTS, n, CHUNK), BF16) for n in sizes]
        + [pltpu.SemaphoreType.DMA((STAGES, SLOTS)), pltpu.SemaphoreType.DMA((STAGES, R_SLOTS))]
    )
    if with_da:
        for begin in (per, 2 * per):
            in_specs.append(pl.BlockSpec((1, d, CHUNK), lambda j, begin=begin: (layer, 0, jnp.clip(j - begin, 0, per - 1))))
        out_specs.append(pl.BlockSpec(memory_space=pl.ANY))
        out_shape.append(jax.ShapeDtypeStruct((tokens, d), F32))
        scratch += [pltpu.VMEM((tokens, d), F32), pltpu.SemaphoreType.DMA]
    return pl.pallas_call(
        functools.partial(gradient_kernel, n_c, per, with_da),
        grid=(n_c + STAGES * LAG,),
        in_specs=in_specs,
        out_specs=out_specs,
        out_shape=out_shape,
        scratch_shapes=scratch,
        compiler_params=params(collective_id=collective_id, has_side_effects=True),
        cost_estimate=pl.CostEstimate(
            flops=(5 if with_da else 3) * 2 * tokens * d * ff, bytes_accessed=2 * (w * tokens * ff + 2 * d * tokens), transcendentals=0
        ),
        name="gradients_da" if with_da else "gradients",
    )(at.reshape(2, 2, d // 2, tokens), b, *(weights or ()))


def adamw(w, m, v, g):
    m = 0.9 * m + 0.1 * g
    v = 0.95 * v + 0.05 * g * g
    step = m * lax.rsqrt(v + 1e-8) + 0.1 * w
    return (w - 0.02 * step).astype(BF16), m, v


def adamw_kernel(first, turn, g_ref, w_ref, m_ref, v_ref, *refs):
    w_out, m_out, v_out = refs[-3:]
    color = lax.rem(pl.program_id(0) + first, len(ORDERS))
    rows = g_ref.shape[2]
    by_order = [owners(o) for o in ORDERS]

    def block(p):
        return g_ref[pick(color, [o[p] for o in by_order]), 0].astype(F32)

    together = 128 // rows if turn else 1
    for p in range(0, GROUP, together):
        g = block(p) if not turn else jnp.concatenate([block(p + i) for i in range(together)], 0).T
        at = slice(p * rows, (p + together) * rows)
        at = (0, slice(None), at) if turn else (0, at)
        w_out[at], m_out[at], v_out[at] = adamw(w_ref[at].astype(F32), m_ref[at], v_ref[at], g)


def update(g, which, first, turn, w, m, v, layer, so_far):
    _, d, ff = w.shape if not turn else (w.shape[0], w.shape[2], w.shape[1])
    rows = g.shape[2]
    spec = pl.BlockSpec((1, CHUNK, d), lambda j: (layer, j, 0)) if turn else pl.BlockSpec((1, d, CHUNK), lambda j: (layer, 0, j))
    more = () if so_far is None else so_far
    return pl.pallas_call(
        functools.partial(adamw_kernel, first, turn),
        grid=(ff // CHUNK,),
        in_specs=[pl.BlockSpec((GROUP, 1, rows, CHUNK), lambda j: (0, which, 0, j)), spec, spec, spec]
        + [pl.BlockSpec(memory_space=pl.ANY)] * len(more),
        out_specs=[spec] * 3,
        out_shape=[jax.ShapeDtypeStruct(w.shape, BF16), jax.ShapeDtypeStruct(w.shape, F32), jax.ShapeDtypeStruct(w.shape, F32)],
        input_output_aliases={4 + i: i for i in range(len(more))},
        compiler_params=params(),
        cost_estimate=pl.CostEstimate(flops=d * ff * 1500, bytes_accessed=22 * d * ff, transcendentals=d * ff),
        name="adamw_turned" if turn else "adamw",
    )(g, w, m, v, *more)


def solution(mesh):
    def step(x, dy, *arrays):
        weights, m, v = (arrays[i : i + 3] for i in (0, 3, 6))
        w_gate, w_up, w_down = weights
        x, dy = x[0], dy[0]
        per = w_gate.shape[2] // CHUNK

        gate, up, mid = forward(x, w_gate, w_up, 0)
        h = down(mid, w_down, x, 0)
        b, at = backward_mid(h, dy, 1, w_down, weights=(w_gate, w_up))
        part, by_a = gradients(at, b, 1, 1, weights=(w_gate, w_up))
        g_1 = lax.all_gather(part, "dp", axis=0)
        by_h = dy + jax.vjp(normed, h)[1](by_a.astype(BF16))[0]
        b, at = backward_mid(x, by_h, 0, w_down, kept=(gate, up))
        (part,) = gradients(at, b, 2, 0)
        g_0a = lax.all_gather(part[:2], "dp", axis=0)
        g_0b = lax.all_gather(part[2:], "dp", axis=0)
        g_1, part = lax.optimization_barrier((g_1, part))

        order = ((2, 0), (0, 1), (1, 2))
        done = {}
        for i, which in order:
            done[i] = update(g_1, which, which * per, i == 2, weights[i], m[i], v[i], 1, None)
        for i, which in order:
            g, at_g = (g_0a, which) if which < 2 else (g_0b, 0)
            done[i] = update(g, at_g, which * per, i == 2, weights[i], m[i], v[i], 0, done[i])
        return tuple(done[i][which] for which in range(3) for i in range(3))

    return jax.shard_map(
        step,
        mesh=mesh,
        in_specs=(P(("rep", "dp"), None, None),) * 2 + (P(None, None, None),) * 9,
        out_specs=(P("rep", None, None),) * 9,
        check_vma=False,
    )
```

```python
import functools

import jax
import jax.numpy as jnp
from jax import lax
from jax.experimental import pallas as pl
from jax.experimental.pallas import tpu as pltpu
from jax.sharding import PartitionSpec as P

MESH = pl.DeviceIdType.MESH
F32, BF16 = jnp.float32, jnp.bfloat16
MIB = 1024 * 1024

CORE, Z0, Z1, Y, X = 1, 2, 4, 8, 16
BITS = (CORE, Z0, Z1, Y, X)
ORDERS = (
    ((CORE, X, Y, Z0, Z1),) * 2,
    ((CORE, Y, X, Z0, Z1),) * 2,
    ((CORE, Z0, X, Y, Z1), (CORE, Z0, Y, X, Z1)),
)
STAGES = 5
GROUP = 1 << STAGES
CHUNK = 512
EARLY = 5
WAIT = 2


def position(order, device):
    return sum(((device // m) % 2) << (STAGES - 1 - i) for i, m in enumerate(order))


def owners(order):
    found = [0] * GROUP
    for device in range(GROUP):
        found[position(order, device)] = device
    return found


def params(limit=61, **more):
    return pltpu.CompilerParams(dimension_semantics=("arbitrary",), vmem_limit_bytes=limit * MIB, **more)


def dot(a, b):
    return jnp.dot(a, b, preferred_element_type=F32)


def dot_nt(a, b):
    return lax.dot_general(a, b, (((1,), (1,)), ((), ())), preferred_element_type=F32)


def once(shape, index):
    return pl.BlockSpec(shape, index, pipeline_mode=pl.Buffered(1))


def norm_in(h):
    wide = h.astype(F32)
    return (wide * lax.rsqrt(jnp.mean(wide**2, -1, keepdims=True) + 1e-6)).astype(BF16)


def turned(j, out_ref, first_ref, second_ref):
    width = out_ref.shape[1]
    at = pl.ds(pl.multiple_of(lax.rem(j, 4) * width, width), width)

    @pl.when(j < 4)
    def _():
        out_ref[0] = first_ref[:, at].T

    @pl.when((j >= 4) & (j < 8))
    def _():
        out_ref[0] = second_ref[:, at].T


def forward_kernel(parts, h_ref, dy_ref, wg_ref, wu_ref, gate_ref, up_ref, mid_ref, at_ref, a_ref):
    t = h_ref.shape[0] // parts
    j = pl.program_id(0)

    @pl.when(j == 0)
    def _():
        for i in range(parts):
            a_ref[i * t : (i + 1) * t] = norm_in(h_ref[i * t : (i + 1) * t])

    turned(j, at_ref, dy_ref, a_ref)
    for i in range(parts):
        rows = slice(i * t, (i + 1) * t)
        gate = dot(a_ref[rows], wg_ref[0])
        up = dot(a_ref[rows], wu_ref[0])
        gate_ref[rows] = gate
        up_ref[rows] = up
        mid_ref[rows] = (jax.nn.silu(gate) * up).astype(BF16)


def forward(h, dy, w_gate, w_up, layer):
    tokens, d = h.shape
    ff = w_gate.shape[2]
    weight = pl.BlockSpec((1, d, CHUNK), lambda j: (layer, 0, j))
    tile = pl.BlockSpec((tokens, CHUNK), lambda j: (0, j))
    whole = once((tokens, d), lambda j: (0, 0))
    turn = lambda j: (jnp.minimum(j // 4, 1), jnp.where(j < 8, lax.rem(j, 4), 3), 0)
    return pl.pallas_call(
        functools.partial(forward_kernel, 2),
        grid=(ff // CHUNK,),
        in_specs=[whole, whole, weight, weight],
        out_specs=[tile, tile, tile, pl.BlockSpec((1, d // 4, tokens), turn)],
        out_shape=[jax.ShapeDtypeStruct((tokens, ff), t) for t in (F32, F32, BF16)] + [jax.ShapeDtypeStruct((2, d, tokens), BF16)],
        scratch_shapes=[pltpu.VMEM((tokens, d), BF16)],
        compiler_params=params(),
        cost_estimate=pl.CostEstimate(flops=4 * tokens * d * ff, bytes_accessed=10 * tokens * ff, transcendentals=tokens * ff),
        name="forward",
    )(h, dy, w_gate, w_up)


def down_kernel(mid_ref, w_ref, h_ref, out_ref, a_ref, at_ref):
    h = h_ref[...] + dot(mid_ref[...], w_ref[0]).astype(BF16)
    a = norm_in(h)
    out_ref[...] = h
    a_ref[...] = a
    at_ref[...] = a.T


def down(mid, w_down, h, layer):
    tokens, ff = mid.shape
    d = h.shape[1]
    rows = 256
    block = pl.BlockSpec((rows, d), lambda i: (i, 0))
    return pl.pallas_call(
        down_kernel,
        grid=(tokens // rows,),
        in_specs=[pl.BlockSpec((rows, ff), lambda i: (i, 0)), once((1, ff, d), lambda i: (layer, 0, 0)), block],
        out_specs=[block, block, pl.BlockSpec((d, rows), lambda i: (0, i))],
        out_shape=[jax.ShapeDtypeStruct(s, BF16) for s in ((tokens, d), (tokens, d), (d, tokens))],
        compiler_params=params(),
        cost_estimate=pl.CostEstimate(flops=2 * tokens * d * ff, bytes_accessed=2 * (tokens + d) * ff, transcendentals=0),
        name="down",
    )(mid, w_down, h)


class Exchange:
    def __init__(self, n_c, orders, rows):
        self.n_c, self.orders, self.rows = n_c, orders, rows
        self.sizes = [2 ** (STAGES - 1 - s) * rows for s in range(STAGES)]
        self.slots = [2 if orders[0][s] == orders[1][s] else 4 for s in range(STAGES)]

    def scratch(self):
        return (
            [pltpu.VMEM((n, CHUNK), BF16) for n in self.sizes]
            + [pltpu.VMEM((n, CHUNK), F32) for n in self.sizes]
            + [pltpu.VMEM((slots, n, CHUNK), BF16) for n, slots in zip(self.sizes, self.slots, strict=True)]
            + [pltpu.SemaphoreType.DMA((STAGES,)), pltpu.SemaphoreType.DMA((STAGES, max(self.slots)))]
        )

    def bind(self, j, bits, out_ref, refs):
        self.j, self.out_ref = j, out_ref
        self.give, self.keep, self.came = refs[:STAGES], refs[STAGES : 2 * STAGES], refs[2 * STAGES : 3 * STAGES]
        self.send_sem, self.recv_sem = refs[3 * STAGES :]
        self.all_bits = bits

    def bit(self, s, c):
        even, odd = (self.all_bits[order[s]] for order in self.orders)
        return even if self.orders[0][s] == self.orders[1][s] else jnp.where(lax.rem(c, 2) == 0, even, odd)

    def peer(self, s, c):
        me = lax.axis_index("dp")
        even, odd = (me + order[s] * (1 - 2 * self.all_bits[order[s]]) for order in self.orders)
        return even if self.orders[0][s] == self.orders[1][s] else jnp.where(lax.rem(c, 2) == 0, even, odd)

    def copy(self, s, c):
        slot = lax.rem(c, self.slots[s])
        return pltpu.make_async_remote_copy(
            src_ref=self.give[s],
            dst_ref=self.came[s].at[slot],
            send_sem=self.send_sem.at[s],
            recv_sem=self.recv_sem.at[s, slot],
            device_id={"dp": self.peer(s, c)},
            device_id_type=MESH,
        )

    def advance(self):
        for s in reversed(range(STAGES)):
            c = self.j - (s + 1)

            @pl.when((c >= 0) & (c < self.n_c))
            def _(s=s, c=c):
                copy = self.copy(s, c)
                copy.wait_send()
                copy.wait_recv()
                keep, came = self.keep[s], self.came[s].at[lax.rem(c, self.slots[s])]
                if s == STAGES - 1:
                    self.out_ref[...] = (keep[...] + came[...].astype(F32)).astype(BF16)
                else:
                    half = self.sizes[s + 1]
                    bit = self.bit(s + 1, c)
                    theirs = pl.ds(pl.multiple_of((1 - bit) * half, half), half)
                    mine = pl.ds(pl.multiple_of(bit * half, half), half)
                    self.give[s + 1][...] = (keep[theirs] + came[theirs].astype(F32)).astype(BF16)
                    self.copy(s + 1, c).start()
                    self.keep[s + 1][...] = keep[mine] + came[mine].astype(F32)

    def put(self, at_ref, b):
        core = self.bit(0, self.j)
        self.give[0][...] = dot(at_ref[1 - core], b).astype(BF16)
        self.copy(0, self.j).start()
        self.keep[0][...] = dot(at_ref[core], b)


class Gather:
    def __init__(self, n, first, load, begin, rows):
        self.n, self.first, self.load, self.begin, self.rows = n, first, load, begin, rows

    def scratch(self):
        return [
            pltpu.VMEM((self.n, self.rows, CHUNK), BF16),
            pltpu.SemaphoreType.DMA((2,)),
            pltpu.SemaphoreType.DMA((STAGES, 2)),
            pltpu.SemaphoreType.DMA((STAGES, self.n)),
        ]

    def bind(self, ex, part_ref, all_ref, refs):
        self.ex, self.part_ref, self.all_ref = ex, part_ref, all_ref
        self.block, self.own_sem, self.send_sem, self.recv_sem = refs

    def region(self, k, t):
        start = sum(self.ex.bit(i, self.first + t) * 2 ** (STAGES - 1 - i) for i in range(STAGES - k))
        return self.all_ref.at[t, pl.ds(pl.multiple_of(start * self.rows, 2**k * self.rows), 2**k * self.rows)]

    def own(self, t):
        slot = lax.rem(t, 2)
        return pltpu.make_async_copy(self.block.at[t], self.region(0, t), self.own_sem.at[slot])

    def copy(self, k, t):
        slot = lax.rem(t, 2)
        return pltpu.make_async_remote_copy(
            src_ref=self.block.at[t] if k == 0 else self.region(k, t),
            dst_ref=self.region(k, t),
            send_sem=self.send_sem.at[k, slot],
            recv_sem=self.recv_sem.at[k, t],
            device_id={"dp": self.ex.peer(STAGES - 1 - k, self.first + t)},
            device_id_type=MESH,
        )

    def advance(self):
        t = self.ex.j - self.load

        @pl.when((t >= 0) & (t < self.n))
        def _():
            self.block[t] = self.part_ref[...]

        for k in reversed(range(STAGES + 1)):
            t = self.ex.j - self.begin - k

            @pl.when((t >= 0) & (t < self.n))
            def _(k=k, t=t):
                if k > 0:
                    copy = self.copy(k - 1, t)
                    copy.wait_send()
                    copy.wait_recv()
                if k == 1:
                    self.own(t).wait()
                if k == 0:
                    self.own(t).start()
                if k < STAGES:
                    self.copy(k, t).start()


def start_exchanges(exchanges, gathers, step, out_refs, part_refs, all_ref, refs):
    me = lax.axis_index("dp")
    bits = {m: lax.rem(lax.div(me, m), 2) for m in BITS}
    n = len(refs) // len(exchanges)
    for i, (ex, g) in enumerate(zip(exchanges, gathers, strict=True)):
        mine = refs[i * n : (i + 1) * n]
        ex.bind(step, bits, out_refs[i], mine[:-4])
        g.bind(ex, part_refs[i], all_ref.at[i], mine[-4:])

    @pl.when(pl.program_id(0) == 0)
    def _():
        barrier = pltpu.get_barrier_semaphore()
        for m in BITS:
            pl.semaphore_signal(barrier, inc=1, device_id={"dp": me + m * (1 - 2 * bits[m])}, device_id_type=MESH)
        pl.semaphore_wait(barrier, len(BITS))


def through(gate, up, by_mid):
    by_mid = by_mid.astype(BF16).astype(F32)
    s = jax.nn.sigmoid(gate)
    silu = gate * s
    return (silu * up).astype(BF16), (by_mid * up * (s * (1 + gate * (1 - s)))).astype(BF16), (by_mid * silu).astype(BF16)


def norm_back(h, dy, by_a):
    wide, by_a = h.astype(F32), by_a.astype(BF16).astype(F32)
    scale = lax.rsqrt(jnp.mean(wide**2, -1, keepdims=True) + 1e-6)
    by_h = by_a * scale - wide * (scale * scale * scale * jnp.mean(by_a * wide, -1, keepdims=True))
    return dy + by_h.astype(BF16)


def first_kernel(
    exchanges, gathers, parts, dy_ref, dyt_ref, at_ref, gate_ref, up_ref, wd_ref, part_ref, early_ref, late_ref, all_ref, mid_ref, by_gate_ref,
    by_up_ref, *refs
):
    down, gate, up = exchanges
    j = pl.program_id(0)
    outs = [early_ref.at[0], early_ref.at[1], late_ref.at[0]]
    start_exchanges(exchanges, gathers, j, outs, [part_ref.at[i] for i in range(3)], all_ref, refs)
    more = j < down.n_c
    t = dy_ref.shape[0] // parts
    gathers[0].advance()
    down.advance()

    @pl.when(more)
    def _():
        for i in range(parts):
            rows = slice(i * t, (i + 1) * t)
            by_mid = dot_nt(dy_ref[rows], wd_ref[0])
            mid_ref[rows], by_gate_ref[rows], by_up_ref[rows] = through(gate_ref[rows], up_ref[rows], by_mid)

    gathers[1].advance()
    gate.advance()

    @pl.when(more)
    def _():
        down.put(dyt_ref.at[0], mid_ref[...])

    gathers[2].advance()
    up.advance()

    @pl.when(more)
    def _():
        gate.put(at_ref.at[0], by_gate_ref[...])
        up.put(at_ref.at[0], by_up_ref[...])


def last_step(j, n_c):
    return jnp.where(j < n_c, j, n_c + lax.div(j - n_c, 2))


def last_kernel(
    exchanges, gathers, parts, dy_ref, dyt_ref, at_ref, wg_ref, wu_ref, wd_ref, a_ref, h_ref, out_ref, all_ref, by_h_ref, by_ht_ref, b_ref, mid_ref,
    buf_ref, acc_ref, sem, *refs
):
    down, gate, up = exchanges
    n_c = down.n_c
    j = pl.program_id(0)
    t = dy_ref.shape[0] // parts
    i = j - n_c
    take_a = pltpu.make_async_copy(a_ref, buf_ref.at[1], sem.at[0])
    save = lambda c: pltpu.make_async_copy(buf_ref.at[0], b_ref.at[c], sem.at[1])
    fetch = lambda i: pltpu.make_async_copy(b_ref.at[n_c - 1 - i], buf_ref.at[lax.rem(i, 2)], sem.at[2])

    @pl.when(j == 0)
    def _():
        take_a.start()

    step = jnp.where((j < n_c) | (lax.rem(i, 2) == 0), last_step(j, n_c), -GROUP)
    outs = [out_ref.at[i] for i in range(3)]
    start_exchanges(exchanges, gathers, step, outs, outs, all_ref, refs)

    @pl.when(j == 0)
    def _():
        take_a.wait()

    @pl.when((j >= 1) & (j <= n_c))
    def _():
        save(j - 1).wait()

    for ex, g in zip(exchanges, gathers, strict=True):
        ex.advance()
        g.advance()

    @pl.when(j < n_c)
    def _():
        for p in range(parts):
            rows = slice(p * t, (p + 1) * t)
            by_mid = dot_nt(dy_ref[rows], wd_ref[0])
            a = buf_ref[1, rows]
            mid_ref[rows], buf_ref[0, rows, :CHUNK], buf_ref[0, rows, CHUNK:] = through(dot(a, wg_ref[0]), dot(a, wu_ref[0]), by_mid)
        save(j).start()
        down.put(dyt_ref.at[0], mid_ref[...])
        gate.put(at_ref.at[0], buf_ref[0, :, :CHUNK])
        up.put(at_ref.at[0], buf_ref[0, :, CHUNK:])

    @pl.when((i >= 0) & (i < n_c))
    def _():
        @pl.when(i >= 1)
        def _():
            fetch(i).wait()

        @pl.when(i < n_c - 1)
        def _():
            fetch(i + 1).start()

        slot = lax.rem(i, 2)
        for p in range(parts):
            rows = slice(p * t, (p + 1) * t)
            term = dot_nt(buf_ref[slot, rows, :CHUNK], wg_ref[0]) + dot_nt(buf_ref[slot, rows, CHUNK:], wu_ref[0])

            @pl.when(i == 0)
            def _():
                acc_ref[rows] = term

            @pl.when(i > 0)
            def _():
                acc_ref[rows] += term

    n = by_h_ref.shape[0]
    block = i - n_c

    @pl.when(block >= 0)
    def _():
        rows = pl.ds(pl.multiple_of(block * n, n), n)
        by_h = norm_back(h_ref[...], dy_ref[rows], acc_ref[rows])
        by_h_ref[...] = by_h
        by_ht_ref[...] = by_h.T


def piece(at, which):
    n, d, tokens = at.shape
    return once((1, 2, d // 2, tokens), lambda j: (which, 0, 0, 0)), at.reshape(n, 2, d // 2, tokens)


def backward(layer, w_down, collective_id, dy, dy_t, a_t, kept=None, part=None, a=None, h=None, weights=None):
    tokens, d = dy.shape
    ff = w_down.shape[1]
    n_c, rows = ff // CHUNK, d // GROUP
    exchanges = [Exchange(n_c, orders, rows) for orders in ORDERS]
    chunks, first, load, begin = (EARLY, 0, STAGES, STAGES + WAIT) if kept is None else (n_c - EARLY, EARLY, 0, 0)
    gathers = [Gather(chunks, first, load, begin, rows) for _ in ORDERS]
    clip = lambda j: jnp.minimum(j, n_c - 1)
    dyt_spec, dy_t = piece(*dy_t)
    at_spec, a_t = piece(*a_t)
    tile = pl.BlockSpec((tokens, CHUNK), lambda j: (0, clip(j)))
    weight = pl.BlockSpec((1, d, CHUNK), lambda j: (layer, 0, jnp.where(j < n_c, j, jnp.maximum(2 * n_c - 1 - j, 0))))
    specs = [once((tokens, d), lambda j: (0, 0)), dyt_spec, at_spec] + ([tile, tile] if kept is not None else [weight, weight])
    specs.append(pl.BlockSpec((1, CHUNK, d), lambda j: (layer, clip(j), 0)))
    args = [dy, dy_t, a_t, *(kept if kept is not None else weights), w_down]
    step = (lambda j: j) if kept is not None else (lambda j: last_step(j, n_c))
    parts = (2, 1) if kept is not None else (3,)
    out_specs = [pl.BlockSpec((n, rows, CHUNK), lambda j: (0, 0, jnp.clip(step(j) - STAGES, 0, n_c - 1))) for n in parts]
    out_specs.append(pl.BlockSpec(memory_space=pl.ANY))
    out_shape = [jax.ShapeDtypeStruct((n, rows, ff), BF16) for n in parts] + [jax.ShapeDtypeStruct((3, chunks, d, CHUNK), BF16)]
    scratch = [pltpu.VMEM((tokens, CHUNK), BF16)]
    if kept is not None:
        specs.append(pl.BlockSpec((3, rows, CHUNK), lambda j: (0, 0, EARLY + jnp.minimum(j, chunks - 1))))
        args.append(part)
        scratch += scratch * 2
        grid = n_c + STAGES
    else:
        n = 256
        grid = 2 * n_c + tokens // n
        block = lambda j: jnp.maximum(j - 2 * n_c, 0)
        specs += [pl.BlockSpec(memory_space=pl.ANY), pl.BlockSpec((n, d), lambda j: (block(j), 0))]
        args += [a, h]
        out_specs += [pl.BlockSpec((n, d), lambda j: (block(j), 0)), pl.BlockSpec((d, n), lambda j: (0, block(j)))]
        out_specs.append(pl.BlockSpec(memory_space=pl.ANY))
        out_shape += [jax.ShapeDtypeStruct((tokens, d), BF16), jax.ShapeDtypeStruct((d, tokens), BF16)]
        out_shape.append(jax.ShapeDtypeStruct((n_c, tokens, 2 * CHUNK), BF16))
        scratch += [pltpu.VMEM((2, tokens, d), BF16), pltpu.VMEM((tokens, d), F32), pltpu.SemaphoreType.DMA((3,))]
    return pl.pallas_call(
        functools.partial(first_kernel if kept is not None else last_kernel, exchanges, gathers, 4 if kept is not None else 2),
        grid=(grid,),
        in_specs=specs,
        out_specs=out_specs,
        out_shape=out_shape,
        scratch_shapes=scratch + [one for ex, g in zip(exchanges, gathers, strict=True) for one in ex.scratch() + g.scratch()],
        compiler_params=params(collective_id=collective_id, has_side_effects=True),
        cost_estimate=pl.CostEstimate(
            flops=(8 if kept is not None else 16) * tokens * d * ff, bytes_accessed=8 * tokens * ff, transcendentals=tokens * ff
        ),
        name="first" if kept is not None else "last",
    )(*args)


def adamw(w, m, v, g):
    m = 0.9 * m + 0.1 * g
    v = 0.95 * v + 0.05 * g * g
    step = m * lax.rsqrt(v + 1e-8) + 0.1 * w
    return (w - 0.02 * step).astype(BF16), m, v


def adamw_kernel(orders, turn, *refs):
    (w_ref, m_ref, v_ref), (w_out, m_out, v_out) = refs[:3], refs[-3:]
    g_refs = refs[3:5] if orders is None else refs[3:4]
    rows = 128
    for p in range(m_ref.shape[2 if turn else 1] // rows):
        at = slice(p * rows, (p + 1) * rows)
        if orders is None:
            early = pl.program_id(0) < EARLY
            g = jnp.where(early, g_refs[0][0, 0, at], g_refs[1][0, 0, at]).astype(F32)
        else:
            n = g_refs[0].shape[2]
            even, odd = (owners(order)[p * rows // n : (p + 1) * rows // n] for order in orders)
            device = lambda a, b: a if a == b else jnp.where(lax.rem(pl.program_id(0), 2) == 0, a, b)
            g = jnp.concatenate([g_refs[0][device(a, b), 0].astype(F32) for a, b in zip(even, odd, strict=True)], 0)
        at = (0, slice(None), at) if turn else (0, at)
        w_out[at], m_out[at], v_out[at] = adamw(w_ref[at].astype(F32), m_ref[at], v_ref[at], g.T if turn else g)


def update(g, which, matrix, w, m, v, layer, so_far):
    turn = matrix == 0
    _, d, ff = w.shape if not turn else (w.shape[0], w.shape[2], w.shape[1])
    spec = pl.BlockSpec((1, CHUNK, d), lambda j: (layer, j, 0)) if turn else pl.BlockSpec((1, d, CHUNK), lambda j: (layer, 0, j))
    more = () if so_far is None else so_far
    if len(g) == 2:
        g_specs = [
            pl.BlockSpec((1, 1, d, CHUNK), lambda j: (which, jnp.minimum(j, EARLY - 1), 0, 0)),
            pl.BlockSpec((1, 1, d, CHUNK), lambda j: (which, jnp.maximum(j - EARLY, 0), 0, 0)),
        ]
    else:
        g_specs = [pl.BlockSpec((GROUP, 1, g[0].shape[2], CHUNK), lambda j: (0, which, 0, j))]
    return pl.pallas_call(
        functools.partial(adamw_kernel, None if len(g) == 2 else ORDERS[matrix], turn),
        grid=(ff // CHUNK,),
        in_specs=[spec, spec, spec] + g_specs + [pl.BlockSpec(memory_space=pl.ANY)] * len(more),
        out_specs=[spec] * 3,
        out_shape=[jax.ShapeDtypeStruct(w.shape, BF16), jax.ShapeDtypeStruct(w.shape, F32), jax.ShapeDtypeStruct(w.shape, F32)],
        input_output_aliases={3 + len(g) + i: i for i in range(len(more))},
        compiler_params=params(),
        cost_estimate=pl.CostEstimate(flops=d * ff * 1500, bytes_accessed=22 * d * ff, transcendentals=d * ff),
        name="adamw_turned" if turn else "adamw",
    )(w, m, v, *g, *more)


def solution(mesh):
    def step(x, dy, *arrays):
        weights, m, v = (arrays[i : i + 3] for i in (0, 3, 6))
        w_gate, w_up, w_down = weights
        x, dy = x[0], dy[0]

        gate, up, mid, at = forward(x, dy, w_gate, w_up, 0)
        h, a, a_t = down(mid, w_down, x, 0)
        part, g_1a, by_h, by_h_t, _ = backward(1, w_down, 1, dy, (at, 0), (a_t[None], 0), a=a, h=h, weights=(w_gate, w_up))
        early, late, g_1b = backward(0, w_down, 2, by_h, (by_h_t[None], 0), (at, 1), kept=(gate, up), part=part)
        g_0a = lax.all_gather(early, "dp", axis=0)
        g_0b = lax.all_gather(late, "dp", axis=0)

        place = (2, 0, 1)
        new = {i: update((g_1a, g_1b), i, i, weights[place[i]], m[place[i]], v[place[i]], 1, None) for i in range(3)}
        g_0a, *_ = lax.optimization_barrier((g_0a, *new.values()))
        for i in range(3):
            g, which = (g_0a, i) if i < 2 else (g_0b, 0)
            if i == 2:
                g, new[0], new[1] = lax.optimization_barrier((g, new[0], new[1]))
            new[i] = update((g,), which, i, weights[place[i]], m[place[i]], v[place[i]], 0, new[i])
        return tuple(new[i][which] for which in range(3) for i in (1, 2, 0))

    return jax.shard_map(
        step,
        mesh=mesh,
        in_specs=(P(("rep", "dp"), None, None),) * 2 + (P(None, None, None),) * 9,
        out_specs=(P("rep", None, None),) * 9,
        check_vma=False,
    )
```

```python
import functools

import jax
import jax.numpy as jnp
from jax import lax
from jax.experimental import pallas as pl
from jax.experimental.pallas import tpu as pltpu
from jax.sharding import PartitionSpec as P

MESH = pl.DeviceIdType.MESH
F32, BF16 = jnp.float32, jnp.bfloat16
MIB = 1024 * 1024

CORE, Z0, Z1, Y, X = 1, 2, 4, 8, 16
BITS = (CORE, Z0, Z1, Y, X)
ORDERS = (
    ((CORE, X, Y, Z0, Z1),) * 2,
    ((CORE, Y, X, Z0, Z1),) * 2,
    ((CORE, Z0, X, Y, Z1), (CORE, Z0, Y, X, Z1)),
)
STAGES = 5
GROUP = 1 << STAGES
CHUNK = 512
EARLY = 5
WAIT = 2
BEGIN = (0, 1, 0)


def position(order, device):
    return sum(((device // m) % 2) << (STAGES - 1 - i) for i, m in enumerate(order))


def owners(order):
    found = [0] * GROUP
    for device in range(GROUP):
        found[position(order, device)] = device
    return found


def params(limit=61, **more):
    return pltpu.CompilerParams(dimension_semantics=("arbitrary",), vmem_limit_bytes=limit * MIB, **more)


def dot(a, b):
    return jnp.dot(a, b, preferred_element_type=F32)


def dot_nt(a, b):
    return lax.dot_general(a, b, (((1,), (1,)), ((), ())), preferred_element_type=F32)


def once(shape, index):
    return pl.BlockSpec(shape, index, pipeline_mode=pl.Buffered(1))


def norm_in(h):
    wide = h.astype(F32)
    return (wide * lax.rsqrt(jnp.mean(wide**2, -1, keepdims=True) + 1e-6)).astype(BF16)


def turned(j, out_ref, first_ref, second_ref):
    width = out_ref.shape[1]
    at = pl.ds(pl.multiple_of(lax.rem(j, 4) * width, width), width)

    @pl.when(j < 4)
    def _():
        out_ref[0] = first_ref[:, at].T

    @pl.when((j >= 4) & (j < 8))
    def _():
        out_ref[0] = second_ref[:, at].T


def forward_kernel(parts, h_ref, dy_ref, wg_ref, wu_ref, gate_ref, up_ref, mid_ref, at_ref, a_ref):
    t = h_ref.shape[0] // parts
    j = pl.program_id(0)

    @pl.when(j == 0)
    def _():
        for i in range(parts):
            a_ref[i * t : (i + 1) * t] = norm_in(h_ref[i * t : (i + 1) * t])

    turned(j, at_ref, dy_ref, a_ref)
    for i in range(parts):
        rows = slice(i * t, (i + 1) * t)
        gate = dot(a_ref[rows], wg_ref[0])
        up = dot(a_ref[rows], wu_ref[0])
        gate_ref[rows] = gate
        up_ref[rows] = up
        mid_ref[rows] = (jax.nn.silu(gate) * up).astype(BF16)


def forward(h, dy, w_gate, w_up, layer):
    tokens, d = h.shape
    ff = w_gate.shape[2]
    weight = pl.BlockSpec((1, d, CHUNK), lambda j: (layer, 0, j))
    tile = pl.BlockSpec((tokens, CHUNK), lambda j: (0, j))
    whole = once((tokens, d), lambda j: (0, 0))
    turn = lambda j: (jnp.minimum(j // 4, 1), jnp.where(j < 8, lax.rem(j, 4), 3), 0)
    return pl.pallas_call(
        functools.partial(forward_kernel, 2),
        grid=(ff // CHUNK,),
        in_specs=[whole, whole, weight, weight],
        out_specs=[tile, tile, tile, pl.BlockSpec((1, d // 4, tokens), turn)],
        out_shape=[jax.ShapeDtypeStruct((tokens, ff), t) for t in (F32, F32, BF16)] + [jax.ShapeDtypeStruct((2, d, tokens), BF16)],
        scratch_shapes=[pltpu.VMEM((tokens, d), BF16)],
        compiler_params=params(),
        cost_estimate=pl.CostEstimate(flops=4 * tokens * d * ff, bytes_accessed=10 * tokens * ff, transcendentals=tokens * ff),
        name="forward",
    )(h, dy, w_gate, w_up)


def down_kernel(mid_ref, w_ref, h_ref, out_ref, a_ref, at_ref):
    h = h_ref[...] + dot(mid_ref[...], w_ref[0]).astype(BF16)
    a = norm_in(h)
    out_ref[...] = h
    a_ref[...] = a
    at_ref[...] = a.T


def down(mid, w_down, h, layer):
    tokens, ff = mid.shape
    d = h.shape[1]
    rows = 256
    block = pl.BlockSpec((rows, d), lambda i: (i, 0))
    return pl.pallas_call(
        down_kernel,
        grid=(tokens // rows,),
        in_specs=[pl.BlockSpec((rows, ff), lambda i: (i, 0)), once((1, ff, d), lambda i: (layer, 0, 0)), block],
        out_specs=[block, block, pl.BlockSpec((d, rows), lambda i: (0, i))],
        out_shape=[jax.ShapeDtypeStruct(s, BF16) for s in ((tokens, d), (tokens, d), (d, tokens))],
        compiler_params=params(),
        cost_estimate=pl.CostEstimate(flops=2 * tokens * d * ff, bytes_accessed=2 * (tokens + d) * ff, transcendentals=0),
        name="down",
    )(mid, w_down, h)


class Exchange:
    def __init__(self, n_c, orders, rows):
        self.n_c, self.orders, self.rows = n_c, orders, rows
        self.sizes = [2 ** (STAGES - 1 - s) * rows for s in range(STAGES)]
        self.slots = [2 if orders[0][s] == orders[1][s] else 4 for s in range(STAGES)]

    def scratch(self):
        return (
            [pltpu.VMEM((n, CHUNK), BF16) for n in self.sizes]
            + [pltpu.VMEM((n, CHUNK), F32) for n in self.sizes]
            + [pltpu.VMEM((slots, n, CHUNK), BF16) for n, slots in zip(self.sizes, self.slots, strict=True)]
            + [pltpu.SemaphoreType.DMA((STAGES,)), pltpu.SemaphoreType.DMA((STAGES, max(self.slots)))]
        )

    def bind(self, j, bits, out_ref, refs):
        self.j, self.out_ref = j, out_ref
        self.give, self.keep, self.came = refs[:STAGES], refs[STAGES : 2 * STAGES], refs[2 * STAGES : 3 * STAGES]
        self.send_sem, self.recv_sem = refs[3 * STAGES :]
        self.all_bits = bits

    def bit(self, s, c):
        even, odd = (self.all_bits[order[s]] for order in self.orders)
        return even if self.orders[0][s] == self.orders[1][s] else jnp.where(lax.rem(c, 2) == 0, even, odd)

    def peer(self, s, c):
        me = lax.axis_index("dp")
        even, odd = (me + order[s] * (1 - 2 * self.all_bits[order[s]]) for order in self.orders)
        return even if self.orders[0][s] == self.orders[1][s] else jnp.where(lax.rem(c, 2) == 0, even, odd)

    def copy(self, s, c):
        slot = lax.rem(c, self.slots[s])
        return pltpu.make_async_remote_copy(
            src_ref=self.give[s],
            dst_ref=self.came[s].at[slot],
            send_sem=self.send_sem.at[s],
            recv_sem=self.recv_sem.at[s, slot],
            device_id={"dp": self.peer(s, c)},
            device_id_type=MESH,
        )

    def advance(self):
        for s in reversed(range(STAGES)):
            c = self.j - (s + 1)

            @pl.when((c >= 0) & (c < self.n_c))
            def _(s=s, c=c):
                copy = self.copy(s, c)
                copy.wait_send()
                copy.wait_recv()
                keep, came = self.keep[s], self.came[s].at[lax.rem(c, self.slots[s])]
                if s == STAGES - 1:
                    self.out_ref[...] = (keep[...] + came[...].astype(F32)).astype(BF16)
                else:
                    half = self.sizes[s + 1]
                    bit = self.bit(s + 1, c)
                    theirs = pl.ds(pl.multiple_of((1 - bit) * half, half), half)
                    mine = pl.ds(pl.multiple_of(bit * half, half), half)
                    self.give[s + 1][...] = (keep[theirs] + came[theirs].astype(F32)).astype(BF16)
                    self.copy(s + 1, c).start()
                    self.keep[s + 1][...] = keep[mine] + came[mine].astype(F32)

    def put(self, at_ref, b):
        core = self.bit(0, self.j)
        self.give[0][...] = dot(at_ref[1 - core], b).astype(BF16)
        self.copy(0, self.j).start()
        self.keep[0][...] = dot(at_ref[core], b)


class Gather:
    def __init__(self, n, first, load, begin, stride, rows):
        self.n, self.first, self.load, self.begin, self.stride, self.rows = n, first, load, begin, stride, rows

    def scratch(self):
        return [
            pltpu.VMEM((self.n, self.rows, CHUNK), BF16),
            pltpu.SemaphoreType.DMA((2,)),
            pltpu.SemaphoreType.DMA((STAGES, 2)),
            pltpu.SemaphoreType.DMA((STAGES, self.n)),
        ]

    def bind(self, ex, part_ref, all_ref, refs):
        self.ex, self.part_ref, self.all_ref = ex, part_ref, all_ref
        self.block, self.own_sem, self.send_sem, self.recv_sem = refs

    def region(self, k, t):
        start = sum(self.ex.bit(i, self.first + t) * 2 ** (STAGES - 1 - i) for i in range(STAGES - k))
        return self.all_ref.at[t, pl.ds(pl.multiple_of(start * self.rows, 2**k * self.rows), 2**k * self.rows)]

    def own(self, t):
        slot = lax.rem(t, 2)
        return pltpu.make_async_copy(self.block.at[t], self.region(0, t), self.own_sem.at[slot])

    def copy(self, k, t):
        slot = lax.rem(t, 2)
        return pltpu.make_async_remote_copy(
            src_ref=self.block.at[t] if k == 0 else self.region(k, t),
            dst_ref=self.region(k, t),
            send_sem=self.send_sem.at[k, slot],
            recv_sem=self.recv_sem.at[k, t],
            device_id={"dp": self.ex.peer(STAGES - 1 - k, self.first + t)},
            device_id_type=MESH,
        )

    def chunk_at(self, step):
        t = lax.div(step, self.stride)
        return t, (step >= 0) & (t < self.n) & (lax.rem(step, self.stride) == 0)

    def advance(self, step):
        t, there = self.chunk_at(step - self.load)

        @pl.when(there)
        def _():
            self.block[t] = self.part_ref[...]

        for k in reversed(range(STAGES + 1)):
            t, there = self.chunk_at(step - self.begin - k)

            @pl.when(there)
            def _(k=k, t=t):
                if k > 0:
                    copy = self.copy(k - 1, t)
                    copy.wait_send()
                    copy.wait_recv()
                if k == 1:
                    self.own(t).wait()
                if k == 0:
                    self.own(t).start()
                if k < STAGES:
                    self.copy(k, t).start()


def start_exchanges(exchanges, gathers, step, out_refs, part_refs, all_ref, refs):
    me = lax.axis_index("dp")
    bits = {m: lax.rem(lax.div(me, m), 2) for m in BITS}
    n = len(refs) // len(exchanges)
    for i, (ex, g) in enumerate(zip(exchanges, gathers, strict=True)):
        mine = refs[i * n : (i + 1) * n]
        ex.bind(step, bits, out_refs[i], mine[:-4])
        g.bind(ex, part_refs[i], all_ref.at[i], mine[-4:])

    @pl.when(pl.program_id(0) == 0)
    def _():
        barrier = pltpu.get_barrier_semaphore()
        for m in BITS:
            pl.semaphore_signal(barrier, inc=1, device_id={"dp": me + m * (1 - 2 * bits[m])}, device_id_type=MESH)
        pl.semaphore_wait(barrier, len(BITS))


def through(gate, up, by_mid):
    by_mid = by_mid.astype(BF16).astype(F32)
    s = jax.nn.sigmoid(gate)
    silu = gate * s
    return (silu * up).astype(BF16), (by_mid * up * (s * (1 + gate * (1 - s)))).astype(BF16), (by_mid * silu).astype(BF16)


def norm_back(h, dy, by_a):
    wide, by_a = h.astype(F32), by_a.astype(BF16).astype(F32)
    scale = lax.rsqrt(jnp.mean(wide**2, -1, keepdims=True) + 1e-6)
    by_h = by_a * scale - wide * (scale * scale * scale * jnp.mean(by_a * wide, -1, keepdims=True))
    return dy + by_h.astype(BF16)


def first_kernel(
    exchanges, gathers, parts, dy_ref, dyt_ref, at_ref, gate_ref, up_ref, wd_ref, part_ref, early_ref, late_ref, all_ref, mid_ref, by_gate_ref,
    by_up_ref, *refs
):
    down, gate, up = exchanges
    j = pl.program_id(0)
    outs = [early_ref.at[0], early_ref.at[1], late_ref.at[0]]
    start_exchanges(exchanges, gathers, j, outs, [part_ref.at[i] for i in range(3)], all_ref, refs)
    more = j < down.n_c
    t = dy_ref.shape[0] // parts
    gathers[0].advance(j)
    down.advance()

    @pl.when(more)
    def _():
        for i in range(parts):
            rows = slice(i * t, (i + 1) * t)
            by_mid = dot_nt(dy_ref[rows], wd_ref[0])
            mid_ref[rows], by_gate_ref[rows], by_up_ref[rows] = through(gate_ref[rows], up_ref[rows], by_mid)

    gathers[1].advance(j)
    gate.advance()

    @pl.when(more)
    def _():
        down.put(dyt_ref.at[0], mid_ref[...])

    gathers[2].advance(j)
    up.advance()

    @pl.when(more)
    def _():
        gate.put(at_ref.at[0], by_gate_ref[...])
        up.put(at_ref.at[0], by_up_ref[...])


def last_step(j, n_c):
    return jnp.where(j < n_c, j, n_c + lax.div(j - n_c, 2))


def last_kernel(
    exchanges, gathers, parts, dy_ref, dyt_ref, at_ref, wg_ref, wu_ref, wd_ref, a_ref, h_ref, out_ref, all_ref, by_h_ref, by_ht_ref, b_ref, mid_ref,
    buf_ref, acc_ref, sem, *refs
):
    down, gate, up = exchanges
    n_c = down.n_c
    j = pl.program_id(0)
    t = dy_ref.shape[0] // parts
    i = j - n_c
    take_a = pltpu.make_async_copy(a_ref, buf_ref.at[1], sem.at[0])
    save = lambda c: pltpu.make_async_copy(buf_ref.at[0], b_ref.at[c], sem.at[1])
    fetch = lambda i: pltpu.make_async_copy(b_ref.at[n_c - 1 - i], buf_ref.at[lax.rem(i, 2)], sem.at[2])

    @pl.when(j == 0)
    def _():
        take_a.start()

    step = jnp.where((j < n_c) | (lax.rem(i, 2) == 0), last_step(j, n_c), -GROUP)
    outs = [out_ref.at[i] for i in range(3)]
    start_exchanges(exchanges, gathers, step, outs, outs, all_ref, refs)

    @pl.when(j == 0)
    def _():
        take_a.wait()

    @pl.when((j >= 1) & (j <= n_c))
    def _():
        save(j - 1).wait()

    for ex, g in zip(exchanges, gathers, strict=True):
        ex.advance()
        g.advance(step)

    @pl.when(j < n_c)
    def _():
        for p in range(parts):
            rows = slice(p * t, (p + 1) * t)
            by_mid = dot_nt(dy_ref[rows], wd_ref[0])
            a = buf_ref[1, rows]
            mid_ref[rows], buf_ref[0, rows, :CHUNK], buf_ref[0, rows, CHUNK:] = through(dot(a, wg_ref[0]), dot(a, wu_ref[0]), by_mid)
        save(j).start()
        down.put(dyt_ref.at[0], mid_ref[...])
        gate.put(at_ref.at[0], buf_ref[0, :, :CHUNK])
        up.put(at_ref.at[0], buf_ref[0, :, CHUNK:])

    @pl.when((i >= 0) & (i < n_c))
    def _():
        @pl.when(i >= 1)
        def _():
            fetch(i).wait()

        @pl.when(i < n_c - 1)
        def _():
            fetch(i + 1).start()

        slot = lax.rem(i, 2)
        for p in range(parts):
            rows = slice(p * t, (p + 1) * t)
            term = dot_nt(buf_ref[slot, rows, :CHUNK], wg_ref[0]) + dot_nt(buf_ref[slot, rows, CHUNK:], wu_ref[0])

            @pl.when(i == 0)
            def _():
                acc_ref[rows] = term

            @pl.when(i > 0)
            def _():
                acc_ref[rows] += term

    n = by_h_ref.shape[0]
    block = i - n_c

    @pl.when(block >= 0)
    def _():
        rows = pl.ds(pl.multiple_of(block * n, n), n)
        by_h = norm_back(h_ref[...], dy_ref[rows], acc_ref[rows])
        by_h_ref[...] = by_h
        by_ht_ref[...] = by_h.T


def piece(at, which):
    n, d, tokens = at.shape
    return once((1, 2, d // 2, tokens), lambda j: (which, 0, 0, 0)), at.reshape(n, 2, d // 2, tokens)


def backward(layer, w_down, collective_id, dy, dy_t, a_t, kept=None, part=None, a=None, h=None, weights=None):
    tokens, d = dy.shape
    ff = w_down.shape[1]
    n_c, rows = ff // CHUNK, d // GROUP
    exchanges = [Exchange(n_c, orders, rows) for orders in ORDERS]
    if kept is None:
        gathers = [Gather(EARLY, 0, STAGES, STAGES + WAIT, 1, rows) for _ in ORDERS]
    else:
        gathers = [Gather(n_c - EARLY, EARLY, begin, begin, 2, rows) for begin in BEGIN]
    chunks = gathers[0].n
    clip = lambda j: jnp.minimum(j, n_c - 1)
    dyt_spec, dy_t = piece(*dy_t)
    at_spec, a_t = piece(*a_t)
    tile = pl.BlockSpec((tokens, CHUNK), lambda j: (0, clip(j)))
    weight = pl.BlockSpec((1, d, CHUNK), lambda j: (layer, 0, jnp.where(j < n_c, j, jnp.maximum(2 * n_c - 1 - j, 0))))
    specs = [once((tokens, d), lambda j: (0, 0)), dyt_spec, at_spec] + ([tile, tile] if kept is not None else [weight, weight])
    specs.append(pl.BlockSpec((1, CHUNK, d), lambda j: (layer, clip(j), 0)))
    args = [dy, dy_t, a_t, *(kept if kept is not None else weights), w_down]
    step = (lambda j: j) if kept is not None else (lambda j: last_step(j, n_c))
    parts = (2, 1) if kept is not None else (3,)
    out_specs = [pl.BlockSpec((n, rows, CHUNK), lambda j: (0, 0, jnp.clip(step(j) - STAGES, 0, n_c - 1))) for n in parts]
    out_specs.append(pl.BlockSpec(memory_space=pl.ANY))
    out_shape = [jax.ShapeDtypeStruct((n, rows, ff), BF16) for n in parts] + [jax.ShapeDtypeStruct((3, chunks, d, CHUNK), BF16)]
    scratch = [pltpu.VMEM((tokens, CHUNK), BF16)]
    if kept is not None:
        specs.append(pl.BlockSpec((3, rows, CHUNK), lambda j: (0, 0, EARLY + jnp.minimum(lax.div(j, 2), chunks - 1))))
        args.append(part)
        scratch += scratch * 2
        grid = n_c + STAGES
    else:
        n = 256
        grid = 2 * n_c + tokens // n
        block = lambda j: jnp.maximum(j - 2 * n_c, 0)
        specs += [pl.BlockSpec(memory_space=pl.ANY), pl.BlockSpec((n, d), lambda j: (block(j), 0))]
        args += [a, h]
        out_specs += [pl.BlockSpec((n, d), lambda j: (block(j), 0)), pl.BlockSpec((d, n), lambda j: (0, block(j)))]
        out_specs.append(pl.BlockSpec(memory_space=pl.ANY))
        out_shape += [jax.ShapeDtypeStruct((tokens, d), BF16), jax.ShapeDtypeStruct((d, tokens), BF16)]
        out_shape.append(jax.ShapeDtypeStruct((n_c, tokens, 2 * CHUNK), BF16))
        scratch += [pltpu.VMEM((2, tokens, d), BF16), pltpu.VMEM((tokens, d), F32), pltpu.SemaphoreType.DMA((3,))]
    return pl.pallas_call(
        functools.partial(first_kernel if kept is not None else last_kernel, exchanges, gathers, 4 if kept is not None else 2),
        grid=(grid,),
        in_specs=specs,
        out_specs=out_specs,
        out_shape=out_shape,
        scratch_shapes=scratch + [one for ex, g in zip(exchanges, gathers, strict=True) for one in ex.scratch() + g.scratch()],
        compiler_params=params(collective_id=collective_id, has_side_effects=True),
        cost_estimate=pl.CostEstimate(
            flops=(8 if kept is not None else 16) * tokens * d * ff, bytes_accessed=8 * tokens * ff, transcendentals=tokens * ff
        ),
        name="first" if kept is not None else "last",
    )(*args)


def adamw(w, m, v, g):
    m = 0.9 * m + 0.1 * g
    v = 0.95 * v + 0.05 * g * g
    step = m * lax.rsqrt(v + 1e-8) + 0.1 * w
    return (w - 0.02 * step).astype(BF16), m, v


def adamw_kernel(orders, turn, *refs):
    (w_ref, m_ref, v_ref), (w_out, m_out, v_out) = refs[:3], refs[-3:]
    g_refs = refs[3:5] if orders is None else refs[3:4]
    rows = 128
    for p in range(m_ref.shape[2 if turn else 1] // rows):
        at = slice(p * rows, (p + 1) * rows)
        if orders is None:
            early = pl.program_id(0) < EARLY
            g = jnp.where(early, g_refs[0][0, 0, at], g_refs[1][0, 0, at]).astype(F32)
        else:
            n = g_refs[0].shape[2]
            even, odd = (owners(order)[p * rows // n : (p + 1) * rows // n] for order in orders)
            device = lambda a, b: a if a == b else jnp.where(lax.rem(pl.program_id(0), 2) == 0, a, b)
            g = jnp.concatenate([g_refs[0][device(a, b), 0].astype(F32) for a, b in zip(even, odd, strict=True)], 0)
        at = (0, slice(None), at) if turn else (0, at)
        w_out[at], m_out[at], v_out[at] = adamw(w_ref[at].astype(F32), m_ref[at], v_ref[at], g.T if turn else g)


def update(g, which, matrix, w, m, v, layer, so_far):
    turn = matrix == 0
    _, d, ff = w.shape if not turn else (w.shape[0], w.shape[2], w.shape[1])
    spec = pl.BlockSpec((1, CHUNK, d), lambda j: (layer, j, 0)) if turn else pl.BlockSpec((1, d, CHUNK), lambda j: (layer, 0, j))
    more = () if so_far is None else so_far
    if len(g) == 2:
        g_specs = [
            pl.BlockSpec((1, 1, d, CHUNK), lambda j: (which, jnp.minimum(j, EARLY - 1), 0, 0)),
            pl.BlockSpec((1, 1, d, CHUNK), lambda j: (which, jnp.maximum(j - EARLY, 0), 0, 0)),
        ]
    else:
        g_specs = [pl.BlockSpec((GROUP, 1, g[0].shape[2], CHUNK), lambda j: (0, which, 0, j))]
    return pl.pallas_call(
        functools.partial(adamw_kernel, None if len(g) == 2 else ORDERS[matrix], turn),
        grid=(ff // CHUNK,),
        in_specs=[spec, spec, spec] + g_specs + [pl.BlockSpec(memory_space=pl.ANY)] * len(more),
        out_specs=[spec] * 3,
        out_shape=[jax.ShapeDtypeStruct(w.shape, BF16), jax.ShapeDtypeStruct(w.shape, F32), jax.ShapeDtypeStruct(w.shape, F32)],
        input_output_aliases={3 + len(g) + i: i for i in range(len(more))},
        compiler_params=params(),
        cost_estimate=pl.CostEstimate(flops=d * ff * 1500, bytes_accessed=22 * d * ff, transcendentals=d * ff),
        name="adamw_turned" if turn else "adamw",
    )(w, m, v, *g, *more)


def solution(mesh):
    def step(x, dy, *arrays):
        weights, m, v = (arrays[i : i + 3] for i in (0, 3, 6))
        w_gate, w_up, w_down = weights
        x, dy = x[0], dy[0]

        gate, up, mid, at = forward(x, dy, w_gate, w_up, 0)
        h, a, a_t = down(mid, w_down, x, 0)
        part, g_1a, by_h, by_h_t, _ = backward(1, w_down, 1, dy, (at, 0), (a_t[None], 0), a=a, h=h, weights=(w_gate, w_up))
        early, late, g_1b = backward(0, w_down, 2, by_h, (by_h_t[None], 0), (at, 1), kept=(gate, up), part=part)
        g_0a = lax.all_gather(early, "dp", axis=0)
        g_0b = lax.all_gather(late, "dp", axis=0)

        place = (2, 0, 1)
        new = {i: update((g_1a, g_1b), i, i, weights[place[i]], m[place[i]], v[place[i]], 1, None) for i in range(3)}
        g_0a, *_ = lax.optimization_barrier((g_0a, *new.values()))
        for i in range(3):
            g, which = (g_0a, i) if i < 2 else (g_0b, 0)
            if i == 2:
                g, new[0], new[1] = lax.optimization_barrier((g, new[0], new[1]))
            new[i] = update((g,), which, i, weights[place[i]], m[place[i]], v[place[i]], 0, new[i])
        return tuple(new[i][which] for which in range(3) for i in (1, 2, 0))

    return jax.shard_map(
        step,
        mesh=mesh,
        in_specs=(P(("rep", "dp"), None, None),) * 2 + (P(None, None, None),) * 9,
        out_specs=(P("rep", None, None),) * 9,
        check_vma=False,
    )
```
